32 devices in a mesh: dp: 16 (over z, x, core), tensor: 2 (over y).
Axes of the slice: x: 2, y: 2, z: 4, core: 2. Of those that a mesh axis runs over, the one named last changes fastest.
Arguments:
- latent: bfloat16 [2, 32768, 1024], P(None, ('dp', 'tensor')), may hold values from -6 to 6
- embedding: bfloat16 [2, 32768, 1024], P(None, ('dp', 'tensor')), may hold values from -6 to 6
- prefix_len: int32 [2, 16], P(None, 'dp'), may hold values from 204 to 1024, as said below
- cotangent: bfloat16 [2, 32768, 1024], P(None, ('dp', 'tensor')), may hold values from -6 to 6
- adapter_w: bfloat16 [2048, 1024], P(('dp', 'tensor')), may hold values from -0.125 to 0.125
- pre_attn_gain: bfloat16 [1024], P(('dp', 'tensor')), may hold values from 0.25 to 1.75
- post_attn_gain: bfloat16 [1024], P(('dp', 'tensor')), may hold values from 0.25 to 1.75
- pre_mlp_gain: bfloat16 [1024], P(('dp', 'tensor')), may hold values from 0.25 to 1.75
- post_mlp_gain: bfloat16 [1024], P(('dp', 'tensor')), may hold values from 0.25 to 1.75
- query_w: bfloat16 [1024, 1024], P('dp', 'tensor'), may hold values from -0.375 to 0.375
- key_w: bfloat16 [1024, 1024], P('dp', 'tensor'), may hold values from -0.1875 to 0.1875
- value_w: bfloat16 [1024, 1024], P('dp', 'tensor'), may hold values from -0.1875 to 0.1875
- output_w: bfloat16 [1024, 1024], P('tensor', 'dp'), may hold values from -0.75 to 0.75
- gate_w: bfloat16 [1024, 2816], P('dp', 'tensor'), may hold values from -0.1875 to 0.1875
- up_w: bfloat16 [1024, 2816], P('dp', 'tensor'), may hold values from -0.1875 to 0.1875
- down_w: bfloat16 [2816, 1024], P('tensor', 'dp'), may hold values from -0.109375 to 0.109375
Outputs:
- layer_out: bfloat16 [2, 32768, 1024], P(None, ('dp', 'tensor'))
- latent_grad: bfloat16 [2, 32768, 1024], P(None, ('dp', 'tensor'))
- embedding_grad: bfloat16 [2, 32768, 1024], P(None, ('dp', 'tensor'))
- adapter_grad: float32 [2048, 1024], P(('dp', 'tensor'))
- pre_attn_grad: float32 [1024], P(('dp', 'tensor'))
- post_attn_grad: float32 [1024], P(('dp', 'tensor'))
- pre_mlp_grad: float32 [1024], P(('dp', 'tensor'))
- post_mlp_grad: float32 [1024], P(('dp', 'tensor'))
- query_grad: float32 [1024, 1024], P('dp', 'tensor')
- key_grad: float32 [1024, 1024], P('dp', 'tensor')
- value_grad: float32 [1024, 1024], P('dp', 'tensor')
- output_grad: float32 [1024, 1024], P('tensor', 'dp')
- gate_grad: float32 [1024, 2816], P('dp', 'tensor')
- up_grad: float32 [1024, 2816], P('dp', 'tensor')
- down_grad: float32 [2816, 1024], P('tensor', 'dp')
The draws below stay inside these ranges and needn't reach their ends.
Inputs may be any that keep to these rules, and one draw needn't show every extreme that they name: `prefix_len`: some sequence has exactly 204 and some exactly 1024.
All inputs are finite; a program needn't handle non-finite values.
Results may differ from the reference program's by a relative error of at most 0.025.
Values may be sent and summed in bfloat16 or wider, within the bound.
A program may use at most 384 MiB of HBM per device.

```python
import jax
import jax.numpy as jnp
from jax import lax

D = 1024
H = 8
HD = 128
FF = 2816
LEN = 2048
MICRO = 2
SEQS = 16
ROWS = 32768


def draw_prefix_len(key, part):
    low_end = LEN // 10
    high_end = LEN // 2
    amount = MICRO * SEQS
    values = jax.random.randint(jax.random.fold_in(key, 11), (amount,), low_end, high_end + 1)
    first_pos = jax.random.randint(jax.random.fold_in(key, 12), (), 0, amount)
    step_pos = jax.random.randint(jax.random.fold_in(key, 13), (), 0, amount - 1)
    second_pos = (first_pos + 1 + step_pos) % amount
    positions = jnp.arange(amount)
    values = jnp.where(positions == first_pos, low_end, values)
    values = jnp.where(positions == second_pos, high_end, values)
    return values.reshape(MICRO, SEQS).astype(jnp.int32)


def levels(key, dims, split, smallest, high):
    level = 1.0
    for axis_at, parts in split:
        heights = jax.random.uniform(jax.random.fold_in(jax.random.fold_in(key, 6), axis_at), (parts,), jnp.float32, smallest / len(split), high / len(split))
        level = level * jnp.repeat(jnp.exp(heights), dims[axis_at] // parts).reshape((-1,) + (1,) * (len(dims) - 1 - axis_at))
    return level


def scatter_about(key, extent, width, bound, pieces=(), kind=jnp.bfloat16):
    level = levels(key, extent, pieces, -0.22, 0.18) if pieces else 1.0
    values = jax.random.normal(key, extent, jnp.float32) * width * level
    return jnp.minimum(jnp.maximum(values, -bound), bound).astype(kind)


def setup_inputs(seed: int = 0) -> dict:
    splits = jax.random.split(jax.random.key(seed), 17)
    return {
        "latent": scatter_about(splits[0], (MICRO, ROWS, D), 1.0, 6.0, ((1, 32),)),
        "embedding": scatter_about(splits[1], (MICRO, ROWS, D), 1.0, 6.0, ((1, 32),)),
        "prefix_len": draw_prefix_len(jax.random.fold_in(splits[16], 71), 0),
        "cotangent": scatter_about(splits[3], (MICRO, ROWS, D), 1.0, 6.0, ((1, 32),)),
        "adapter_w": scatter_about(splits[4], (2 * D, D), (2 * D) ** -0.5, 0.125, ((0, 32),)),
        "pre_attn_gain": jnp.clip(1.0 + 0.15 * jax.random.normal(splits[5], (D,), jnp.float32), 0.25, 1.75).astype(jnp.bfloat16),
        "post_attn_gain": jnp.clip(1.0 + 0.15 * jax.random.normal(splits[6], (D,), jnp.float32), 0.25, 1.75).astype(jnp.bfloat16),
        "pre_mlp_gain": jnp.clip(1.0 + 0.15 * jax.random.normal(splits[7], (D,), jnp.float32), 0.25, 1.75).astype(jnp.bfloat16),
        "post_mlp_gain": jnp.clip(1.0 + 0.15 * jax.random.normal(splits[8], (D,), jnp.float32), 0.25, 1.75).astype(jnp.bfloat16),
        "query_w": scatter_about(splits[9], (D, H * HD), (D // 4) ** -0.5, 0.375, ((0, 16), (1, 2))),
        "key_w": scatter_about(splits[10], (D, H * HD), D ** -0.5, 0.1875, ((0, 16), (1, 2))),
        "value_w": scatter_about(splits[11], (D, H * HD), D ** -0.5, 0.1875, ((0, 16), (1, 2))),
        "output_w": scatter_about(splits[12], (H * HD, D), (H * HD // 16) ** -0.5, 0.75, ((0, 2), (1, 16))),
        "gate_w": scatter_about(splits[13], (D, FF), D ** -0.5, 0.1875, ((0, 16), (1, 2))),
        "up_w": scatter_about(splits[14], (D, FF), D ** -0.5, 0.1875, ((0, 16), (1, 2))),
        "down_w": scatter_about(splits[15], (FF, D), FF ** -0.5, 0.109375, ((0, 2), (1, 16))),
    }


HIGHEST = lax.Precision.HIGHEST
EPS = 1e-06
THETA = 50000.0

@jax.custom_vjp
def low(v):
    return lax.optimization_barrier(v.astype(jnp.bfloat16)).astype(jnp.float32)

@jax.custom_vjp
def low_back(v):
    return v

def low_keep(v):
    return (low(v), None)

def low_pass(kept, grad):
    return (grad,)

def back_keep(v):
    return (v, None)

def back_low(kept, grad):
    return (low(grad),)
low.defvjp(low_keep, low_pass)
low_back.defvjp(back_keep, back_low)

def matmul(left, right):
    return jnp.dot(left, right, precision=HIGHEST)

def rms_norm(values, gain):
    factor = lax.rsqrt(lax.optimization_barrier(jnp.mean(values * values, axis=-1, keepdims=True)) + EPS)
    return values * factor * gain

def rotary_tables(length):
    half_dim = HD // 2
    inv_freq = THETA ** (-(jnp.arange(half_dim, dtype=jnp.float32) * 2.0 / HD))
    angles = jnp.arange(length, dtype=jnp.float32)[:, None] * inv_freq[None, :]
    return (jnp.cos(angles), jnp.sin(angles))

def rotate(values_in, cosine, sine_tab):
    half_dim = values_in.shape[-1] // 2
    leading = values_in[..., :half_dim]
    trailing = values_in[..., half_dim:]
    cos_b = cosine[:, None, :]
    sin_b = sine_tab[:, None, :]
    return jnp.concatenate([leading * cos_b - trailing * sin_b, trailing * cos_b + leading * sin_b], axis=-1)

def attention(queries, key_rows, value_rows, prefix_end):
    length = queries.shape[0]
    block_len = min(512, length)
    blocks = length // block_len
    scaling = HD ** (-0.5)
    key_pos = jnp.arange(length, dtype=jnp.int32)

    def one_block(block_idx):
        offset = (block_idx * block_len).astype(jnp.int32)
        query_blk = lax.dynamic_slice_in_dim(queries, offset, block_len, 0)
        scores = jnp.einsum('qhd,khd->hqk', query_blk, key_rows, precision=HIGHEST) * scaling
        scores = low_back(scores)
        query_pos = offset + jnp.arange(block_len, dtype=jnp.int32)
        allowed = (key_pos[None, :] <= query_pos[:, None]) | (key_pos[None, :] < prefix_end)
        scores = jnp.where(allowed[None], scores, -1e+30)
        weights = low(jax.nn.softmax(scores, axis=-1))
        return jnp.einsum('hqk,khd->qhd', weights, value_rows, precision=HIGHEST)
    outputs = lax.map(jax.checkpoint(one_block), jnp.arange(blocks, dtype=jnp.int32))
    return outputs.reshape(length, H * HD)

def core_layer(latent_seq, embed_seq, prefix_end, parameters):
    adapter, gain_a, gain_b, gain_c, gain_d, w_query, w_key, w_value, w_output, w_gate, w_up, w_down = parameters
    length = latent_seq.shape[0]
    joined = low(jnp.concatenate([latent_seq, embed_seq], axis=-1))
    residual = low_back(matmul(joined, adapter))
    attn_in = low(rms_norm(residual, gain_a))
    cosine, sine_tab = rotary_tables(length)
    queries = low_back(matmul(attn_in, w_query)).reshape(length, H, HD)
    keys_raw = low_back(matmul(attn_in, w_key)).reshape(length, H, HD)
    value_rows = low(low_back(matmul(attn_in, w_value))).reshape(length, H, HD)
    queries = low(rotate(queries, cosine, sine_tab))
    keys_rot = low(rotate(keys_raw, cosine, sine_tab))
    attn = low(low_back(attention(queries, keys_rot, value_rows, prefix_end)))
    attn_proj = low_back(matmul(attn, w_output))
    middle = residual + rms_norm(attn_proj, gain_b)
    mlp_in = low(rms_norm(middle, gain_c))
    gate_act = low_back(matmul(mlp_in, w_gate))
    up_act = low_back(matmul(mlp_in, w_up))
    hidden = low(jax.nn.silu(gate_act) * up_act)
    mlp_proj = low_back(matmul(hidden, w_down))
    return middle + rms_norm(mlp_proj, gain_d)

def reference(latent, embedding, prefix_len, cotangent, adapter_w, pre_attn_gain, post_attn_gain, pre_mlp_gain, post_mlp_gain, query_w, key_w, value_w, output_w, gate_w, up_w, down_w):
    parameters = (adapter_w.astype(jnp.float32), pre_attn_gain.astype(jnp.float32), post_attn_gain.astype(jnp.float32), pre_mlp_gain.astype(jnp.float32), post_mlp_gain.astype(jnp.float32), query_w.astype(jnp.float32), key_w.astype(jnp.float32), value_w.astype(jnp.float32), output_w.astype(jnp.float32), gate_w.astype(jnp.float32), up_w.astype(jnp.float32), down_w.astype(jnp.float32))
    seq_total = MICRO * SEQS
    lat_seqs = latent.astype(jnp.float32).reshape(seq_total, LEN, D)
    emb_seqs = embedding.astype(jnp.float32).reshape(seq_total, LEN, D)
    cot_seqs = cotangent.astype(jnp.float32).reshape(seq_total, LEN, D)
    prefix_flat = prefix_len.reshape(seq_total).astype(jnp.int32)

    def step(carry, items):
        lat_one, emb_one, cot_one, prefix_one = items

        def forward(lat_in, emb_in, params_in):
            return core_layer(lat_in, emb_in, prefix_one, params_in)
        result, pullback = jax.vjp(forward, lat_one, emb_one, parameters)
        lat_grad, emb_grad, param_grads = pullback(cot_one)
        carry = jax.tree.map(lambda left, right: left + right, carry, param_grads)
        return (carry, (result, lat_grad, emb_grad))
    zeros = jax.tree.map(jnp.zeros_like, parameters)
    totals, stacked = lax.scan(step, zeros, (lat_seqs, emb_seqs, cot_seqs, prefix_flat))
    results, lat_grads, emb_grads = stacked
    layer_out = results.reshape(MICRO, ROWS, D).astype(jnp.bfloat16)
    latent_grad = lat_grads.reshape(MICRO, ROWS, D).astype(jnp.bfloat16)
    embedding_grad = emb_grads.reshape(MICRO, ROWS, D).astype(jnp.bfloat16)
    return (layer_out, latent_grad, embedding_grad, totals[0], totals[1], totals[2], totals[3], totals[4], totals[5], totals[6], totals[7], totals[8], totals[9], totals[10], totals[11])
```

```python
import functools

import jax
import jax.numpy as jnp
from jax import lax
from jax.experimental import pallas as pl
from jax.experimental.pallas import tpu as pltpu
from jax.sharding import PartitionSpec as P

HD = 128
LEN = 2048


EPS = 1e-06
THETA = 50000.0


def inner(left, right):
    return lax.dot_general(
        left, right, (((0,), (0,)), ((), ())), preferred_element_type=jnp.float32
    )


def outer_t(left, right):
    return lax.dot_general(
        left, right, (((1,), (1,)), ((), ())), preferred_element_type=jnp.float32
    )


def product(left, right):
    return jnp.dot(left, right, preferred_element_type=jnp.float32)


def normalize(values):
    factor = lax.rsqrt(jnp.mean(values * values, axis=-1, keepdims=True) + EPS)
    return (values * factor, factor)


def norm_back(scaled_grad, unit_rows, factor):
    return factor * (
        scaled_grad - unit_rows * jnp.mean(scaled_grad * unit_rows, axis=-1, keepdims=True)
    )


def rotary_tables(row_total):
    half_dim = HD // 2
    inv_freq = THETA ** (-(jnp.arange(half_dim, dtype=jnp.float32) * 2.0 / HD))
    positions = (jnp.arange(row_total, dtype=jnp.int32) % LEN).astype(jnp.float32)
    angles = positions[:, None] * inv_freq[None, :]
    return (jnp.cos(angles)[:, None, :], jnp.sin(angles)[:, None, :])


def rotate(values_in, cosine, sine_tab):
    half_dim = values_in.shape[-1] // 2
    leading = values_in[..., :half_dim]
    trailing = values_in[..., half_dim:]
    return jnp.concatenate(
        [leading * cosine - trailing * sine_tab, trailing * cosine + leading * sine_tab], axis=-1
    )


def rotate_back(values_in, cosine, sine_tab):
    half_dim = values_in.shape[-1] // 2
    leading = values_in[..., :half_dim]
    trailing = values_in[..., half_dim:]
    return jnp.concatenate(
        [leading * cosine + trailing * sine_tab, trailing * cosine - leading * sine_tab], axis=-1
    )


def masked_scores(query_blk, key_rows, block_idx, block_len, prefix_end):
    scaling = HD ** (-0.5)
    scores = (
        jnp.einsum("qhd,khd->hqk", query_blk, key_rows, preferred_element_type=jnp.float32)
        * scaling
    )
    key_pos = jnp.arange(LEN, dtype=jnp.int32)
    query_pos = block_idx * block_len + jnp.arange(block_len, dtype=jnp.int32)
    allowed = (key_pos[None, :] <= query_pos[:, None]) | (key_pos[None, :] < prefix_end)
    return jnp.where(allowed[None], scores, -1e30)


def attend(queries, keys_rot, value_rows, prefix_seq):
    row_total, head_count, head_dim = queries.shape
    seq_count = row_total // LEN
    block_len = min(512, LEN)
    blocks = LEN // block_len

    def one_seq(items):
        seq_idx, prefix_end = items

        def one_block(block_idx):
            query_blk = lax.dynamic_slice_in_dim(
                queries, seq_idx * LEN + block_idx * block_len, block_len, 0
            )
            scores = masked_scores(query_blk, keys_rot, block_idx, block_len, prefix_end)
            row_max = jnp.max(scores, axis=-1, keepdims=True)
            expo = jnp.exp(scores - row_max)
            row_sum = jnp.sum(expo, axis=-1, keepdims=True)
            weights = (expo / row_sum).astype(jnp.bfloat16)
            attn_blk = jnp.einsum(
                "hqk,khd->qhd", weights, value_rows, preferred_element_type=jnp.float32
            )
            return (attn_blk, (row_max + jnp.log(row_sum))[..., 0])

        attn_seq, lse_seq = lax.map(one_block, jnp.arange(blocks, dtype=jnp.int32))
        return (
            attn_seq.reshape(LEN, head_count * head_dim),
            jnp.transpose(lse_seq, (1, 0, 2)).reshape(head_count, LEN),
        )

    attn_all, lse_all = lax.map(one_seq, (jnp.arange(seq_count, dtype=jnp.int32), prefix_seq))
    return (attn_all.reshape(row_total, head_count * head_dim), lse_all)


def attend_back(queries, keys_rot, value_rows, lse_all, grad_attn, prefix_seq):
    row_total, head_count, head_dim = queries.shape
    seq_count = row_total // LEN
    block_len = min(512, LEN)
    blocks = LEN // block_len
    scaling = HD ** (-0.5)

    def one_seq(items):
        seq_idx, prefix_end, lse_seq = items

        def one_block(carry, block_idx):
            grad_key_acc, grad_val_acc = carry
            offset = seq_idx * LEN + block_idx * block_len
            query_blk = lax.dynamic_slice_in_dim(queries, offset, block_len, 0)
            grad_blk = lax.dynamic_slice_in_dim(grad_attn, offset, block_len, 0)
            scores = masked_scores(query_blk, keys_rot, block_idx, block_len, prefix_end)
            lse_blk = lax.dynamic_slice_in_dim(lse_seq, block_idx * block_len, block_len, 1)
            weights = jnp.exp(scores - lse_blk[..., None])
            grad_weights = jnp.einsum(
                "qhd,khd->hqk", grad_blk, value_rows, preferred_element_type=jnp.float32
            )
            row_dot = jnp.sum(weights * grad_weights, axis=-1, keepdims=True)
            grad_scores = (weights * (grad_weights - row_dot)).astype(jnp.bfloat16)
            grad_query = (
                jnp.einsum(
                    "hqk,khd->qhd", grad_scores, keys_rot, preferred_element_type=jnp.float32
                )
                * scaling
            )
            grad_key_acc = (
                grad_key_acc
                + jnp.einsum(
                    "hqk,qhd->khd", grad_scores, query_blk, preferred_element_type=jnp.float32
                )
                * scaling
            )
            grad_val_acc = grad_val_acc + jnp.einsum(
                "hqk,qhd->khd",
                weights.astype(jnp.bfloat16),
                grad_blk,
                preferred_element_type=jnp.float32,
            )
            return ((grad_key_acc, grad_val_acc), grad_query)

        zeros = jnp.zeros((LEN, head_count, head_dim), jnp.float32)
        sums, grad_queries = lax.scan(
            one_block, (zeros, zeros), jnp.arange(blocks, dtype=jnp.int32)
        )
        return (grad_queries.reshape(LEN, head_count, head_dim), sums[0], sums[1])

    grad_q, grad_k, grad_v = lax.map(
        one_seq, (jnp.arange(seq_count, dtype=jnp.int32), prefix_seq, lse_all)
    )
    shape = (row_total, head_count, head_dim)
    return (grad_q.reshape(shape), grad_k.reshape(shape), grad_v.reshape(shape))


def gather_weights(local_weights):
    (
        adapter_w,
        pre_attn_gain,
        post_attn_gain,
        pre_mlp_gain,
        post_mlp_gain,
        query_w,
        key_w,
        value_w,
        output_w,
        gate_w,
        up_w,
        down_w,
    ) = local_weights
    adapter_part = (
        lax.all_gather(adapter_w, ("dp", "tensor"), axis=0, tiled=True),
        lax.all_gather(pre_attn_gain, ("dp", "tensor"), axis=0, tiled=True),
        lax.all_gather(post_attn_gain, ("dp", "tensor"), axis=0, tiled=True),
        lax.all_gather(pre_mlp_gain, ("dp", "tensor"), axis=0, tiled=True),
        lax.all_gather(post_mlp_gain, ("dp", "tensor"), axis=0, tiled=True),
    )
    attn_part = (
        lax.all_gather(query_w, "dp", axis=0, tiled=True),
        lax.all_gather(key_w, "dp", axis=0, tiled=True),
        lax.all_gather(value_w, "dp", axis=0, tiled=True),
        lax.all_gather(output_w, "dp", axis=1, tiled=True),
    )
    mlp_part = (
        lax.all_gather(gate_w, "dp", axis=0, tiled=True),
        lax.all_gather(up_w, "dp", axis=0, tiled=True),
        lax.all_gather(down_w, "dp", axis=1, tiled=True),
    )
    return tuple(adapter_part) + tuple(attn_part) + tuple(mlp_part)


def micro_step(lat_rows, emb_rows, prefix_seq, cot_rows, gathered):
    (
        adapter_full,
        gain_one,
        gain_two,
        gain_three,
        gain_four,
        query_full,
        key_full,
        value_full,
        output_full,
        gate_full,
        up_full,
        down_full,
    ) = gathered
    gain_a = gain_one.astype(jnp.float32)
    gain_b = gain_two.astype(jnp.float32)
    gain_c = gain_three.astype(jnp.float32)
    gain_d = gain_four.astype(jnp.float32)
    joined = jnp.concatenate([lat_rows, emb_rows], axis=1)
    residual = product(joined, adapter_full)
    unit_one, factor_one = normalize(residual)
    attn_in = lax.all_gather((unit_one * gain_a).astype(jnp.bfloat16), "tensor", axis=0, tiled=True)
    row_total = attn_in.shape[0]
    head_count = query_full.shape[1] // HD
    cosine, sine_tab = rotary_tables(row_total)
    queries = rotate(
        product(attn_in, query_full).reshape(row_total, head_count, HD), cosine, sine_tab
    ).astype(jnp.bfloat16)
    keys_rot = rotate(
        product(attn_in, key_full).reshape(row_total, head_count, HD), cosine, sine_tab
    ).astype(jnp.bfloat16)
    value_rows = (
        product(attn_in, value_full).astype(jnp.bfloat16).reshape(row_total, head_count, HD)
    )
    attn_full, lse_all = attend(queries, keys_rot, value_rows, prefix_seq)
    attn_low = attn_full.astype(jnp.bfloat16)
    attn_proj = lax.psum_scatter(
        product(attn_low, output_full).astype(jnp.bfloat16),
        "tensor",
        scatter_dimension=0,
        tiled=True,
    ).astype(jnp.float32)
    unit_two, factor_two = normalize(attn_proj)
    middle = residual + unit_two * gain_b
    unit_three, factor_three = normalize(middle)
    mlp_in = lax.all_gather(
        (unit_three * gain_c).astype(jnp.bfloat16), "tensor", axis=0, tiled=True
    )
    gate_act = product(mlp_in, gate_full)
    up_act = product(mlp_in, up_full)
    hidden = (jax.nn.silu(gate_act) * up_act).astype(jnp.bfloat16)
    mlp_proj = lax.psum_scatter(
        product(hidden, down_full).astype(jnp.bfloat16), "tensor", scatter_dimension=0, tiled=True
    ).astype(jnp.float32)
    unit_four, factor_four = normalize(mlp_proj)
    result = middle + unit_four * gain_d
    grad_out = cot_rows.astype(jnp.float32)
    post_mlp_part = jnp.sum(grad_out * unit_four, axis=0)
    grad_mlp = norm_back(grad_out * gain_d, unit_four, factor_four).astype(jnp.bfloat16)
    grad_mlp_all = lax.all_gather(grad_mlp, "tensor", axis=0, tiled=True)
    down_part = inner(hidden, grad_mlp_all)
    grad_hidden = outer_t(grad_mlp_all, down_full)
    sigma = jax.nn.sigmoid(gate_act)
    grad_gate = (grad_hidden * up_act * sigma * (1.0 + gate_act * (1.0 - sigma))).astype(
        jnp.bfloat16
    )
    grad_up = (grad_hidden * gate_act * sigma).astype(jnp.bfloat16)
    gate_part = inner(mlp_in, grad_gate)
    up_part = inner(mlp_in, grad_up)
    grad_mlp_in = lax.psum_scatter(
        (outer_t(grad_gate, gate_full) + outer_t(grad_up, up_full)).astype(jnp.bfloat16),
        "tensor",
        scatter_dimension=0,
        tiled=True,
    ).astype(jnp.float32)
    pre_mlp_part = jnp.sum(grad_mlp_in * unit_three, axis=0)
    grad_middle = grad_out + norm_back(grad_mlp_in * gain_c, unit_three, factor_three)
    post_attn_part = jnp.sum(grad_middle * unit_two, axis=0)
    grad_proj = norm_back(grad_middle * gain_b, unit_two, factor_two).astype(jnp.bfloat16)
    grad_proj_all = lax.all_gather(grad_proj, "tensor", axis=0, tiled=True)
    output_part = inner(attn_low, grad_proj_all)
    grad_attn = (
        outer_t(grad_proj_all, output_full).astype(jnp.bfloat16).reshape(row_total, head_count, HD)
    )
    grad_q, grad_k, grad_v = attend_back(
        queries, keys_rot, value_rows, lse_all, grad_attn, prefix_seq
    )
    grad_q_raw = (
        rotate_back(grad_q, cosine, sine_tab)
        .astype(jnp.bfloat16)
        .reshape(row_total, head_count * HD)
    )
    grad_k_raw = (
        rotate_back(grad_k, cosine, sine_tab)
        .astype(jnp.bfloat16)
        .reshape(row_total, head_count * HD)
    )
    grad_values = grad_v.astype(jnp.bfloat16).reshape(row_total, head_count * HD)
    query_part = inner(attn_in, grad_q_raw)
    key_part = inner(attn_in, grad_k_raw)
    value_part = inner(attn_in, grad_values)
    grad_attn_in_part = (
        outer_t(grad_q_raw, query_full)
        + outer_t(grad_k_raw, key_full)
        + outer_t(grad_values, value_full)
    )
    grad_attn_in = lax.psum_scatter(
        grad_attn_in_part.astype(jnp.bfloat16), "tensor", scatter_dimension=0, tiled=True
    ).astype(jnp.float32)
    pre_attn_part = jnp.sum(grad_attn_in * unit_one, axis=0)
    grad_residual = (grad_middle + norm_back(grad_attn_in * gain_a, unit_one, factor_one)).astype(
        jnp.bfloat16
    )
    adapter_part = inner(joined, grad_residual)
    grad_joined = outer_t(grad_residual, adapter_full)
    width = lat_rows.shape[1]
    latent_grad = grad_joined[:, :width].astype(jnp.bfloat16)
    embedding_grad = grad_joined[:, width:].astype(jnp.bfloat16)
    partials = (
        adapter_part,
        pre_attn_part,
        post_attn_part,
        pre_mlp_part,
        post_mlp_part,
        query_part,
        key_part,
        value_part,
        output_part,
        gate_part,
        up_part,
        down_part,
    )
    return (result.astype(jnp.bfloat16), latent_grad, embedding_grad, partials)


def local(
    latent,
    embedding,
    prefix_len,
    cotangent,
    adapter_w,
    pre_attn_gain,
    post_attn_gain,
    pre_mlp_gain,
    post_mlp_gain,
    query_w,
    key_w,
    value_w,
    output_w,
    gate_w,
    up_w,
    down_w,
):
    local_weights = (
        adapter_w,
        pre_attn_gain,
        post_attn_gain,
        pre_mlp_gain,
        post_mlp_gain,
        query_w,
        key_w,
        value_w,
        output_w,
        gate_w,
        up_w,
        down_w,
    )
    batches = latent.shape[0]
    layer_rows = []
    latent_rows = []
    embed_rows = []
    totals = None
    for micro in range(batches):
        current = gather_weights(local_weights)
        result, lat_grad, emb_grad, partials = micro_step(
            latent[micro], embedding[micro], prefix_len[micro], cotangent[micro], current
        )
        layer_rows.append(result)
        latent_rows.append(lat_grad)
        embed_rows.append(emb_grad)
        if totals is None:
            totals = partials
        else:
            totals = jax.tree.map(lambda left, right: left + right, totals, partials)
    adapter_grad, pre_attn_grad, post_attn_grad, pre_mlp_grad, post_mlp_grad = (
        lax.psum_scatter(totals[0], ("dp", "tensor"), scatter_dimension=0, tiled=True),
        lax.psum_scatter(totals[1], ("dp", "tensor"), scatter_dimension=0, tiled=True),
        lax.psum_scatter(totals[2], ("dp", "tensor"), scatter_dimension=0, tiled=True),
        lax.psum_scatter(totals[3], ("dp", "tensor"), scatter_dimension=0, tiled=True),
        lax.psum_scatter(totals[4], ("dp", "tensor"), scatter_dimension=0, tiled=True),
    )
    query_grad, key_grad, value_grad, output_grad = (
        lax.psum_scatter(
            totals[5].astype(jnp.bfloat16), "dp", scatter_dimension=0, tiled=True
        ).astype(jnp.float32),
        lax.psum_scatter(
            totals[6].astype(jnp.bfloat16), "dp", scatter_dimension=0, tiled=True
        ).astype(jnp.float32),
        lax.psum_scatter(
            totals[7].astype(jnp.bfloat16), "dp", scatter_dimension=0, tiled=True
        ).astype(jnp.float32),
        lax.psum_scatter(
            totals[8].astype(jnp.bfloat16), "dp", scatter_dimension=1, tiled=True
        ).astype(jnp.float32),
    )
    gate_grad, up_grad, down_grad = (
        lax.psum_scatter(
            totals[9].astype(jnp.bfloat16), "dp", scatter_dimension=0, tiled=True
        ).astype(jnp.float32),
        lax.psum_scatter(
            totals[10].astype(jnp.bfloat16), "dp", scatter_dimension=0, tiled=True
        ).astype(jnp.float32),
        lax.psum_scatter(
            totals[11].astype(jnp.bfloat16), "dp", scatter_dimension=1, tiled=True
        ).astype(jnp.float32),
    )
    return (
        jnp.stack(layer_rows),
        jnp.stack(latent_rows),
        jnp.stack(embed_rows),
        adapter_grad,
        pre_attn_grad,
        post_attn_grad,
        pre_mlp_grad,
        post_mlp_grad,
        query_grad,
        key_grad,
        value_grad,
        output_grad,
        gate_grad,
        up_grad,
        down_grad,
    )


BLK = 512
LOG2E = 1.4426950408889634
NEG = -1e30


def turn(values, cosine, signed_sine):
    return values * cosine + pltpu.roll(values, HD // 2, 1) * signed_sine


def visible(row_start, key_start, row_axis, prefix_end):
    rows = row_start + lax.broadcasted_iota(jnp.int32, (BLK, BLK), row_axis)
    keys = key_start + lax.broadcasted_iota(jnp.int32, (BLK, BLK), 1 - row_axis)
    return (keys <= rows) | (keys < prefix_end)


def attend_kernel(
    info, q_own, q_oth, k_own, k_oth, v_own, v_oth, cos_ref, sin_ref,
    attn_ref, lse_ref, q_ref, k_ref, v_ref, wide, acc, peak,
):
    side, prefix_end = info[0], info[1]
    half = q_own.shape[0]
    length = 2 * half
    blocks = length // BLK
    factor = LOG2E * HD**-0.5

    def stored(block):
        return pl.multiple_of(lax.rem(block * BLK + side * half, length), BLK)

    for slot, (q_in, k_in, v_in) in enumerate(((q_own, k_own, v_own), (q_oth, k_oth, v_oth))):
        place = side if slot == 0 else 1 - side
        rows = pl.ds(pl.multiple_of(place * half, half), half)
        cosine, signed_sine = cos_ref[rows, :], sin_ref[rows, :]
        here = pl.ds(slot * half, half)
        q_ref[here, :] = turn(q_in[...], cosine, signed_sine).astype(jnp.bfloat16)
        k_ref[here, :] = turn(k_in[...], cosine, signed_sine).astype(jnp.bfloat16)
        v_ref[here, :] = v_in[...]
        wide[here, :HD] = v_in[...]
        wide[here, HD:] = jnp.ones((half, HD), jnp.bfloat16)

    for row_block in range(blocks):
        mine = pl.ds(stored(row_block), BLK)
        acc[...] = jnp.zeros_like(acc)
        peak[...] = jnp.full_like(peak, NEG)

        def step(key_block, masked):
            keys = pl.ds(stored(key_block), BLK)
            scores = outer_t(q_ref[mine, :], k_ref[keys, :]) * factor
            if masked:
                seen = visible(row_block * BLK, key_block * BLK, 0, prefix_end)
                scores = jnp.where(seen, scores, NEG)
            old = peak[:, :1]
            top = jnp.maximum(old, jnp.max(scores, axis=1, keepdims=True))
            weights = jnp.exp2(scores - top).astype(jnp.bfloat16)
            acc[...] = acc[...] * jnp.exp2(old - top) + product(weights, wide[keys, :])
            peak[...] = jnp.broadcast_to(top, peak.shape)

        clear = jnp.maximum(row_block, prefix_end // BLK)
        last = jnp.maximum(row_block + 1, (prefix_end + BLK - 1) // BLK)

        def plain(key_block, carry):
            step(key_block, False)
            return carry

        def edged(key_block, carry):
            step(key_block, True)
            return carry

        lax.fori_loop(0, clear, plain, 0)
        lax.fori_loop(clear, last, edged, 0)
        total = acc[:, HD:]
        attn_ref[mine, :] = (acc[:, :HD] / total).astype(jnp.bfloat16)
        lse_ref[0, :, mine] = jnp.transpose(peak[...] + jnp.log2(total))[:8]


def attend_back_kernel(
    info, q_ref, k_ref, v_ref, attn_ref, lse_ref, go_own, go_oth, cos_ref, sin_ref,
    grad_ref, go_ref, delta, dq, dk, dv,
):
    side, prefix_end = info[0], info[1]
    head = pl.program_id(0)
    heads = grad_ref.shape[1] // (3 * HD)
    half = go_own.shape[0]
    length = 2 * half
    blocks = length // BLK
    factor = LOG2E * HD**-0.5
    scaling = HD**-0.5

    def stored(block):
        return pl.multiple_of(lax.rem(block * BLK + side * half, length), BLK)

    go_ref[:half, :] = go_own[...]
    go_ref[half:, :] = go_oth[...]
    for block in range(blocks):
        here = pl.ds(block * BLK, BLK)
        both = go_ref[here, :].astype(jnp.float32) * attn_ref[here, :].astype(jnp.float32)
        sums = jnp.sum(jnp.transpose(both), axis=0, keepdims=True)
        delta[:, here] = jnp.broadcast_to(sums, (8, BLK))
    dq[...] = jnp.zeros_like(dq)

    for key_block in range(blocks):
        keys = pl.ds(stored(key_block), BLK)
        dk[...] = jnp.zeros_like(dk)
        dv[...] = jnp.zeros_like(dv)

        def step(row_block, masked):
            rows = pl.ds(stored(row_block), BLK)
            queries, grads = q_ref[rows, :], go_ref[rows, :]
            scores = outer_t(k_ref[keys, :], queries) * factor - lse_ref[0, :1, rows]
            if masked:
                seen = visible(row_block * BLK, key_block * BLK, 1, prefix_end)
                scores = jnp.where(seen, scores, NEG)
            weights = jnp.exp2(scores)
            slope = outer_t(v_ref[keys, :], grads) - delta[:1, rows]
            low = (weights * slope).astype(jnp.bfloat16)
            dv[...] += product(weights.astype(jnp.bfloat16), grads)
            dk[...] += product(low, queries)
            dq[rows, :] += inner(low, k_ref[keys, :])

        whole = (key_block + 1) * BLK <= prefix_end
        reached = key_block * BLK < prefix_end
        first = jnp.where(reached, 0, key_block)
        clear = jnp.where(whole, 0, key_block + 1)

        def plain(row_block, carry):
            step(row_block, False)
            return carry

        def edged(row_block, carry):
            step(row_block, True)
            return carry

        lax.fori_loop(first, clear, edged, 0)
        lax.fori_loop(clear, blocks, plain, 0)
        place = pl.ds(pl.multiple_of(key_block * BLK, BLK), BLK)
        back = turn(dk[...] * scaling, cos_ref[place, :], -sin_ref[place, :])
        columns = pl.ds(pl.multiple_of((heads + head) * HD, HD), HD)
        grad_ref[keys, columns] = back.astype(jnp.bfloat16)
        columns = pl.ds(pl.multiple_of((2 * heads + head) * HD, HD), HD)
        grad_ref[keys, columns] = dv[...].astype(jnp.bfloat16)

    for block in range(blocks):
        rows = pl.ds(stored(block), BLK)
        place = pl.ds(block * BLK, BLK)
        back = turn(dq[rows, :] * scaling, cos_ref[place, :], -sin_ref[place, :])
        columns = pl.ds(pl.multiple_of(head * HD, HD), HD)
        grad_ref[rows, columns] = back.astype(jnp.bfloat16)


def head_columns(rows, shift=0):
    return pl.BlockSpec((rows, HD), lambda head, info: (0, head + shift))


def fixed(rows, columns):
    return pl.BlockSpec((rows, columns), lambda head, info: (0, 0))


def attend_half(info, qk_own, qk_oth, v_own, v_oth, tables):
    half = qk_own.shape[0]
    heads = v_own.shape[1] // HD
    length = 2 * half
    low = jax.ShapeDtypeStruct((length, heads * HD), jnp.bfloat16)
    pairs = heads * length * length * 0.6
    return pl.pallas_call(
        attend_kernel,
        grid_spec=pltpu.PrefetchScalarGridSpec(
            num_scalar_prefetch=1,
            grid=(heads,),
            in_specs=[
                head_columns(half), head_columns(half),
                head_columns(half, heads), head_columns(half, heads),
                head_columns(half), head_columns(half),
                fixed(length, HD), fixed(length, HD),
            ],
            out_specs=[
                head_columns(length),
                pl.BlockSpec((1, 8, length), lambda head, info: (head, 0, 0)),
                head_columns(length), head_columns(length), head_columns(length),
            ],
            scratch_shapes=[
                pltpu.VMEM((length, 2 * HD), jnp.bfloat16),
                pltpu.VMEM((BLK, 2 * HD), jnp.float32),
                pltpu.VMEM((BLK, HD), jnp.float32),
            ],
        ),
        out_shape=(low, jax.ShapeDtypeStruct((heads, 8, length), jnp.float32), low, low, low),
        cost_estimate=pl.CostEstimate(
            flops=int(pairs * 8 * HD), bytes_accessed=int(40 * length * heads * HD), transcendentals=int(pairs)
        ),
        name="attend",
    )(info, qk_own, qk_oth, qk_own, qk_oth, v_own, v_oth, *tables)


def attend_back_half(info, saved, go_own, go_oth, tables):
    attn, lse, queries, keys_rot, value_rows = saved
    half = go_own.shape[0]
    heads = go_own.shape[1] // HD
    length = 2 * half
    pairs = heads * length * length * 0.6
    return pl.pallas_call(
        attend_back_kernel,
        grid_spec=pltpu.PrefetchScalarGridSpec(
            num_scalar_prefetch=1,
            grid=(heads,),
            in_specs=[
                head_columns(length), head_columns(length), head_columns(length), head_columns(length),
                pl.BlockSpec((1, 8, length), lambda head, info: (head, 0, 0)),
                head_columns(half), head_columns(half),
                fixed(length, HD), fixed(length, HD),
            ],
            out_specs=fixed(length, 3 * heads * HD),
            scratch_shapes=[
                pltpu.VMEM((length, HD), jnp.bfloat16),
                pltpu.VMEM((8, length), jnp.float32),
                pltpu.VMEM((length, HD), jnp.float32),
                pltpu.VMEM((BLK, HD), jnp.float32),
                pltpu.VMEM((BLK, HD), jnp.float32),
            ],
        ),
        out_shape=jax.ShapeDtypeStruct((length, 3 * heads * HD), jnp.bfloat16),
        cost_estimate=pl.CostEstimate(
            flops=int(pairs * 20 * HD), bytes_accessed=int(16 * length * heads * HD), transcendentals=int(pairs)
        ),
        name="attend_back",
    )(info, queries, keys_rot, value_rows, attn, lse, go_own, go_oth, *tables)


def swap(values):
    return lax.ppermute(values, "tensor", [(0, 1), (1, 0)])


def low(values):
    return values.astype(jnp.bfloat16)


def total_over(parts, side):
    mine = lax.psum_scatter(parts, "dp", scatter_dimension=0, tiled=True)
    width = mine.shape[1] // 2
    lower, upper = mine[:, :width], mine[:, width:]
    sent = jnp.where(side == 0, upper, lower)
    kept = jnp.where(side == 0, lower, upper)
    return kept.astype(jnp.float32) + swap(sent).astype(jnp.float32)


def fast_local(
    latent, embedding, prefix_len, cotangent, adapter_w, pre_attn_gain, post_attn_gain,
    pre_mlp_gain, post_mlp_gain, query_w, key_w, value_w, output_w, gate_w, up_w, down_w,
):
    side = lax.axis_index("tensor")
    dp_size, both = lax.axis_size("dp"), ("dp", "tensor")
    half, width = latent.shape[1:]
    shard = adapter_w.shape[0]
    gain_len = pre_attn_gain.shape[0]
    quarter = query_w.shape[1]
    inner_len = gate_w.shape[1]

    gains_row = jnp.concatenate([pre_attn_gain, post_attn_gain, pre_mlp_gain, post_mlp_gain])
    gains_block = jnp.pad(gains_row[None, :], ((0, shard - 1), (0, 0)))
    first = lax.all_gather(jnp.concatenate([adapter_w, gains_block], axis=1), both, axis=0, tiled=True)
    attn_w = lax.all_gather(
        jnp.concatenate([query_w, key_w, value_w, output_w.T], axis=1), ("tensor", "dp"), axis=0, tiled=True
    ).reshape(2, width, -1)
    mlp_w = lax.all_gather(
        jnp.concatenate([gate_w, up_w, down_w.T], axis=1), ("tensor", "dp"), axis=0, tiled=True
    ).reshape(2, width, -1)
    adapter_top, adapter_bottom = first[:width, :width], first[width:, :width]
    gains = first[::shard, width:].reshape(-1, 4, gain_len).transpose(1, 0, 2).reshape(4, width)
    gain_a, gain_b, gain_c, gain_d = (gains[i].astype(jnp.float32) for i in range(4))

    info = jnp.stack([side.astype(jnp.int32), jnp.where(side == 0, prefix_len[0, 0], prefix_len[1, 0])])
    half_dim = HD // 2
    inv_freq = THETA ** (-(jnp.arange(half_dim, dtype=jnp.float32) * 2.0 / HD))
    angles = jnp.arange(2 * half, dtype=jnp.float32)[:, None] * inv_freq[None, :]
    cosine, sine = jnp.cos(angles), jnp.sin(angles)
    tables = (jnp.concatenate([cosine, cosine], axis=1), jnp.concatenate([-sine, sine], axis=1))

    def pick(values, index):
        return lax.dynamic_index_in_dim(values, index, 0, keepdims=False)

    order = (side, 1 - side)
    lat = [pick(latent, i) for i in order]
    emb = [pick(embedding, i) for i in order]
    cot = [pick(cotangent, i) for i in order]

    def enter(slot):
        residual = product(lat[slot], adapter_top) + product(emb[slot], adapter_bottom)
        unit, factor = normalize(residual)
        return residual, unit, factor, low(unit * gain_a)

    res_o, unit_one_o, factor_one_o, attn_in_sent = enter(1)
    attn_in_oth = swap(attn_in_sent)
    res_m, unit_one_m, factor_one_m, attn_in_own = enter(0)

    def project(rows, part):
        weights = attn_w[part]
        return (
            product(rows, weights[:, : 2 * quarter]),
            low(product(rows, weights[:, 2 * quarter : 3 * quarter])),
        )

    own = [project(attn_in_own, part) for part in range(2)]
    oth = [project(attn_in_oth, part) for part in range(2)]
    saved = [
        attend_half(info, own[p][0], oth[p][0], own[p][1], oth[p][1], tables) for p in range(2)
    ]
    out_w = [attn_w[p][:, 3 * quarter :] for p in range(2)]

    def project_out(rows):
        return outer_t(saved[0][0][rows], out_w[0]) + outer_t(saved[1][0][rows], out_w[1])

    proj_o = swap(low(project_out(slice(half, None)))).astype(jnp.float32)
    proj_m = low(project_out(slice(0, half))).astype(jnp.float32)

    gate_w_all = [mlp_w[p][:, :inner_len] for p in range(2)]
    up_w_all = [mlp_w[p][:, inner_len : 2 * inner_len] for p in range(2)]
    down_w_all = [mlp_w[p][:, 2 * inner_len :] for p in range(2)]

    def feed(residual, attn_proj, cot_rows):
        unit_two, factor_two = normalize(attn_proj)
        middle = residual + unit_two * gain_b
        unit_three, factor_three = normalize(middle)
        mlp_in = low(unit_three * gain_c)
        acts = []
        mlp_proj = None
        for p in range(2):
            gate_act = product(mlp_in, gate_w_all[p])
            up_act = product(mlp_in, up_w_all[p])
            hidden = low(jax.nn.silu(gate_act) * up_act)
            acts.append((gate_act, up_act, hidden))
            part = outer_t(hidden, down_w_all[p])
            mlp_proj = part if mlp_proj is None else mlp_proj + part
        unit_four, factor_four = normalize(mlp_proj)
        result = low(middle + unit_four * gain_d)
        grad_out = cot_rows.astype(jnp.float32)
        post_mlp_part = jnp.sum(grad_out * unit_four, axis=0)
        grad_mlp = low(norm_back(grad_out * gain_d, unit_four, factor_four))
        grads = []
        grad_mlp_in = None
        for p in range(2):
            gate_act, up_act, hidden = acts[p]
            grad_hidden = product(grad_mlp, down_w_all[p])
            sigma = jax.nn.sigmoid(gate_act)
            grad_gate = low(grad_hidden * up_act * sigma * (1.0 + gate_act * (1.0 - sigma)))
            grad_up = low(grad_hidden * gate_act * sigma)
            grads.append((grad_gate, grad_up, hidden))
            part = outer_t(grad_gate, gate_w_all[p]) + outer_t(grad_up, up_w_all[p])
            grad_mlp_in = part if grad_mlp_in is None else grad_mlp_in + part
        pre_mlp_part = jnp.sum(grad_mlp_in * unit_three, axis=0)
        grad_middle = grad_out + norm_back(grad_mlp_in * gain_c, unit_three, factor_three)
        post_attn_part = jnp.sum(grad_middle * unit_two, axis=0)
        grad_proj = low(norm_back(grad_middle * gain_b, unit_two, factor_two))
        return result, grad_middle, grad_proj, mlp_in, grad_mlp, grads, (
            post_attn_part, pre_mlp_part, post_mlp_part,
        )

    result_m, grad_middle_m, grad_proj_own, mlp_in_m, grad_mlp_m, grads_m, sums_m = feed(
        res_m, proj_m, cot[0]
    )
    result_o, grad_middle_o, grad_proj_sent, mlp_in_o, grad_mlp_o, grads_o, sums_o = feed(
        res_o, proj_o, cot[1]
    )
    grad_proj_oth = swap(grad_proj_sent)
    mlp_cols = []
    for p in range(2):
        for i in range(2):
            mlp_cols.append(low(inner(mlp_in_m, grads_m[p][i]) + inner(mlp_in_o, grads_o[p][i])))
        mlp_cols.append(low(inner(grad_mlp_m, grads_m[p][2]) + inner(grad_mlp_o, grads_o[p][2])))
    mlp_total = total_over(jnp.concatenate(mlp_cols, axis=1), side)

    grad_qkv = []
    for p in range(2):
        go_own = low(product(grad_proj_own, out_w[p]))
        go_oth = low(product(grad_proj_oth, out_w[p]))
        grad_qkv.append(attend_back_half(info, saved[p], go_own, go_oth, tables))

    in_w = [attn_w[p][:, : 3 * quarter] for p in range(2)]

    def grad_in(rows):
        return outer_t(grad_qkv[0][rows], in_w[0]) + outer_t(grad_qkv[1][rows], in_w[1])

    grad_in_o = swap(low(grad_in(slice(half, None)))).astype(jnp.float32)
    grad_in_m = low(grad_in(slice(0, half))).astype(jnp.float32)
    attn_cols = []
    for p in range(2):
        mine, others = slice(0, half), slice(half, None)
        attn_cols.append(
            low(inner(attn_in_own, grad_qkv[p][mine]) + inner(attn_in_oth, grad_qkv[p][others]))
        )
        attn_cols.append(
            low(inner(grad_proj_own, saved[p][0][mine]) + inner(grad_proj_oth, saved[p][0][others]))
        )
    attn_total = total_over(jnp.concatenate(attn_cols, axis=1), side)

    def leave(grad_attn_in, unit_one, factor_one, grad_middle):
        part = jnp.sum(grad_attn_in * unit_one, axis=0)
        grad_residual = low(grad_middle + norm_back(grad_attn_in * gain_a, unit_one, factor_one))
        return (
            grad_residual, part,
            low(outer_t(grad_residual, adapter_top)), low(outer_t(grad_residual, adapter_bottom)),
        )

    grad_res_m, pre_m, lat_grad_m, emb_grad_m = leave(grad_in_m, unit_one_m, factor_one_m, grad_middle_m)
    grad_res_o, pre_o, lat_grad_o, emb_grad_o = leave(grad_in_o, unit_one_o, factor_one_o, grad_middle_o)
    top = low(inner(lat[0], grad_res_m) + inner(lat[1], grad_res_o))
    bottom = low(inner(emb[0], grad_res_m) + inner(emb[1], grad_res_o))
    gain_sums = jnp.stack([pre_m + pre_o] + [sums_m[i] + sums_o[i] for i in range(3)])
    gain_sums = low(gain_sums).reshape(4, -1, gain_len).transpose(1, 0, 2).reshape(-1, 1, 4 * gain_len)
    gain_sums = jnp.pad(gain_sums, ((0, 0), (0, shard - 1), (0, 0))).reshape(-1, 4 * gain_len)
    last = jnp.concatenate([jnp.concatenate([top, bottom], axis=0), gain_sums], axis=1)
    last = lax.psum_scatter(last, "dp", scatter_dimension=0, tiled=True)
    sent = jnp.where(side == 0, last[shard:], last[:shard])
    kept = jnp.where(side == 0, last[:shard], last[shard:])
    last = kept.astype(jnp.float32) + swap(sent).astype(jnp.float32)
    gain_grads = [last[0, width + i * gain_len : width + (i + 1) * gain_len] for i in range(4)]

    def join(mine, others):
        return jnp.stack([jnp.where(side == 0, mine, others), jnp.where(side == 0, others, mine)])

    return (
        join(result_m, result_o),
        join(lat_grad_m, lat_grad_o),
        join(emb_grad_m, emb_grad_o),
        last[:, :width],
        *gain_grads,
        attn_total[:, :quarter],
        attn_total[:, quarter : 2 * quarter],
        attn_total[:, 2 * quarter : 3 * quarter],
        attn_total[:, 3 * quarter :].T,
        mlp_total[:, :inner_len],
        mlp_total[:, inner_len : 2 * inner_len],
        mlp_total[:, 2 * inner_len :].T,
    )


def choose(*arguments):
    latent, prefix_len, query_w = arguments[0], arguments[2], arguments[9]
    paired = lax.axis_size("tensor") == 2 and latent.shape[0] == 2
    whole = 2 * latent.shape[1] == LEN and prefix_len.shape[1] == 1 and query_w.shape[1] % HD == 0
    return fast_local(*arguments) if paired and whole else local(*arguments)


def solution(mesh):
    placed = (
        P(None, ("dp", "tensor"), None),
        P(None, ("dp", "tensor"), None),
        P(None, "dp"),
        P(None, ("dp", "tensor"), None),
        P(("dp", "tensor"), None),
        P(("dp", "tensor")),
        P(("dp", "tensor")),
        P(("dp", "tensor")),
        P(("dp", "tensor")),
        P("dp", "tensor"),
        P("dp", "tensor"),
        P("dp", "tensor"),
        P("tensor", "dp"),
        P("dp", "tensor"),
        P("dp", "tensor"),
        P("tensor", "dp"),
    )
    return jax.shard_map(
        choose,
        mesh=mesh,
        in_specs=placed,
        out_specs=(
            P(None, ("dp", "tensor"), None),
            P(None, ("dp", "tensor"), None),
            P(None, ("dp", "tensor"), None),
            P(("dp", "tensor"), None),
            P(("dp", "tensor")),
            P(("dp", "tensor")),
            P(("dp", "tensor")),
            P(("dp", "tensor")),
            P("dp", "tensor"),
            P("dp", "tensor"),
            P("dp", "tensor"),
            P("tensor", "dp"),
            P("dp", "tensor"),
            P("dp", "tensor"),
            P("tensor", "dp"),
        ),
        check_vma=False,
    )
```

```python
import functools

import jax
import jax.numpy as jnp
from jax import lax
from jax.experimental import pallas as pl
from jax.experimental.pallas import tpu as pltpu
from jax.experimental.layout import Layout, with_layout_constraint
from jax.sharding import PartitionSpec as P

HD = 128
LEN = 2048


EPS = 1e-06
THETA = 50000.0


def inner(left, right):
    return lax.dot_general(
        left, right, (((0,), (0,)), ((), ())), preferred_element_type=jnp.float32
    )


def outer_t(left, right):
    return lax.dot_general(
        left, right, (((1,), (1,)), ((), ())), preferred_element_type=jnp.float32
    )


def product(left, right):
    return jnp.dot(left, right, preferred_element_type=jnp.float32)


def normalize(values):
    factor = lax.rsqrt(jnp.mean(values * values, axis=-1, keepdims=True) + EPS)
    return (values * factor, factor)


def norm_back(scaled_grad, unit_rows, factor):
    return factor * (
        scaled_grad - unit_rows * jnp.mean(scaled_grad * unit_rows, axis=-1, keepdims=True)
    )


def rotary_tables(row_total):
    half_dim = HD // 2
    inv_freq = THETA ** (-(jnp.arange(half_dim, dtype=jnp.float32) * 2.0 / HD))
    positions = (jnp.arange(row_total, dtype=jnp.int32) % LEN).astype(jnp.float32)
    angles = positions[:, None] * inv_freq[None, :]
    return (jnp.cos(angles)[:, None, :], jnp.sin(angles)[:, None, :])


def rotate(values_in, cosine, sine_tab):
    half_dim = values_in.shape[-1] // 2
    leading = values_in[..., :half_dim]
    trailing = values_in[..., half_dim:]
    return jnp.concatenate(
        [leading * cosine - trailing * sine_tab, trailing * cosine + leading * sine_tab], axis=-1
    )


def rotate_back(values_in, cosine, sine_tab):
    half_dim = values_in.shape[-1] // 2
    leading = values_in[..., :half_dim]
    trailing = values_in[..., half_dim:]
    return jnp.concatenate(
        [leading * cosine + trailing * sine_tab, trailing * cosine - leading * sine_tab], axis=-1
    )


def masked_scores(query_blk, key_rows, block_idx, block_len, prefix_end):
    scaling = HD ** (-0.5)
    scores = (
        jnp.einsum("qhd,khd->hqk", query_blk, key_rows, preferred_element_type=jnp.float32)
        * scaling
    )
    key_pos = jnp.arange(LEN, dtype=jnp.int32)
    query_pos = block_idx * block_len + jnp.arange(block_len, dtype=jnp.int32)
    allowed = (key_pos[None, :] <= query_pos[:, None]) | (key_pos[None, :] < prefix_end)
    return jnp.where(allowed[None], scores, -1e30)


def attend(queries, keys_rot, value_rows, prefix_seq):
    row_total, head_count, head_dim = queries.shape
    seq_count = row_total // LEN
    block_len = min(512, LEN)
    blocks = LEN // block_len

    def one_seq(items):
        seq_idx, prefix_end = items

        def one_block(block_idx):
            query_blk = lax.dynamic_slice_in_dim(
                queries, seq_idx * LEN + block_idx * block_len, block_len, 0
            )
            scores = masked_scores(query_blk, keys_rot, block_idx, block_len, prefix_end)
            row_max = jnp.max(scores, axis=-1, keepdims=True)
            expo = jnp.exp(scores - row_max)
            row_sum = jnp.sum(expo, axis=-1, keepdims=True)
            weights = (expo / row_sum).astype(jnp.bfloat16)
            attn_blk = jnp.einsum(
                "hqk,khd->qhd", weights, value_rows, preferred_element_type=jnp.float32
            )
            return (attn_blk, (row_max + jnp.log(row_sum))[..., 0])

        attn_seq, lse_seq = lax.map(one_block, jnp.arange(blocks, dtype=jnp.int32))
        return (
            attn_seq.reshape(LEN, head_count * head_dim),
            jnp.transpose(lse_seq, (1, 0, 2)).reshape(head_count, LEN),
        )

    attn_all, lse_all = lax.map(one_seq, (jnp.arange(seq_count, dtype=jnp.int32), prefix_seq))
    return (attn_all.reshape(row_total, head_count * head_dim), lse_all)


def attend_back(queries, keys_rot, value_rows, lse_all, grad_attn, prefix_seq):
    row_total, head_count, head_dim = queries.shape
    seq_count = row_total // LEN
    block_len = min(512, LEN)
    blocks = LEN // block_len
    scaling = HD ** (-0.5)

    def one_seq(items):
        seq_idx, prefix_end, lse_seq = items

        def one_block(carry, block_idx):
            grad_key_acc, grad_val_acc = carry
            offset = seq_idx * LEN + block_idx * block_len
            query_blk = lax.dynamic_slice_in_dim(queries, offset, block_len, 0)
            grad_blk = lax.dynamic_slice_in_dim(grad_attn, offset, block_len, 0)
            scores = masked_scores(query_blk, keys_rot, block_idx, block_len, prefix_end)
            lse_blk = lax.dynamic_slice_in_dim(lse_seq, block_idx * block_len, block_len, 1)
            weights = jnp.exp(scores - lse_blk[..., None])
            grad_weights = jnp.einsum(
                "qhd,khd->hqk", grad_blk, value_rows, preferred_element_type=jnp.float32
            )
            row_dot = jnp.sum(weights * grad_weights, axis=-1, keepdims=True)
            grad_scores = (weights * (grad_weights - row_dot)).astype(jnp.bfloat16)
            grad_query = (
                jnp.einsum(
                    "hqk,khd->qhd", grad_scores, keys_rot, preferred_element_type=jnp.float32
                )
                * scaling
            )
            grad_key_acc = (
                grad_key_acc
                + jnp.einsum(
                    "hqk,qhd->khd", grad_scores, query_blk, preferred_element_type=jnp.float32
                )
                * scaling
            )
            grad_val_acc = grad_val_acc + jnp.einsum(
                "hqk,qhd->khd",
                weights.astype(jnp.bfloat16),
                grad_blk,
                preferred_element_type=jnp.float32,
            )
            return ((grad_key_acc, grad_val_acc), grad_query)

        zeros = jnp.zeros((LEN, head_count, head_dim), jnp.float32)
        sums, grad_queries = lax.scan(
            one_block, (zeros, zeros), jnp.arange(blocks, dtype=jnp.int32)
        )
        return (grad_queries.reshape(LEN, head_count, head_dim), sums[0], sums[1])

    grad_q, grad_k, grad_v = lax.map(
        one_seq, (jnp.arange(seq_count, dtype=jnp.int32), prefix_seq, lse_all)
    )
    shape = (row_total, head_count, head_dim)
    return (grad_q.reshape(shape), grad_k.reshape(shape), grad_v.reshape(shape))


def gather_weights(local_weights):
    (
        adapter_w,
        pre_attn_gain,
        post_attn_gain,
        pre_mlp_gain,
        post_mlp_gain,
        query_w,
        key_w,
        value_w,
        output_w,
        gate_w,
        up_w,
        down_w,
    ) = local_weights
    adapter_part = (
        lax.all_gather(adapter_w, ("dp", "tensor"), axis=0, tiled=True),
        lax.all_gather(pre_attn_gain, ("dp", "tensor"), axis=0, tiled=True),
        lax.all_gather(post_attn_gain, ("dp", "tensor"), axis=0, tiled=True),
        lax.all_gather(pre_mlp_gain, ("dp", "tensor"), axis=0, tiled=True),
        lax.all_gather(post_mlp_gain, ("dp", "tensor"), axis=0, tiled=True),
    )
    attn_part = (
        lax.all_gather(query_w, "dp", axis=0, tiled=True),
        lax.all_gather(key_w, "dp", axis=0, tiled=True),
        lax.all_gather(value_w, "dp", axis=0, tiled=True),
        lax.all_gather(output_w, "dp", axis=1, tiled=True),
    )
    mlp_part = (
        lax.all_gather(gate_w, "dp", axis=0, tiled=True),
        lax.all_gather(up_w, "dp", axis=0, tiled=True),
        lax.all_gather(down_w, "dp", axis=1, tiled=True),
    )
    return tuple(adapter_part) + tuple(attn_part) + tuple(mlp_part)


def micro_step(lat_rows, emb_rows, prefix_seq, cot_rows, gathered):
    (
        adapter_full,
        gain_one,
        gain_two,
        gain_three,
        gain_four,
        query_full,
        key_full,
        value_full,
        output_full,
        gate_full,
        up_full,
        down_full,
    ) = gathered
    gain_a = gain_one.astype(jnp.float32)
    gain_b = gain_two.astype(jnp.float32)
    gain_c = gain_three.astype(jnp.float32)
    gain_d = gain_four.astype(jnp.float32)
    joined = jnp.concatenate([lat_rows, emb_rows], axis=1)
    residual = product(joined, adapter_full)
    unit_one, factor_one = normalize(residual)
    attn_in = lax.all_gather((unit_one * gain_a).astype(jnp.bfloat16), "tensor", axis=0, tiled=True)
    row_total = attn_in.shape[0]
    head_count = query_full.shape[1] // HD
    cosine, sine_tab = rotary_tables(row_total)
    queries = rotate(
        product(attn_in, query_full).reshape(row_total, head_count, HD), cosine, sine_tab
    ).astype(jnp.bfloat16)
    keys_rot = rotate(
        product(attn_in, key_full).reshape(row_total, head_count, HD), cosine, sine_tab
    ).astype(jnp.bfloat16)
    value_rows = (
        product(attn_in, value_full).astype(jnp.bfloat16).reshape(row_total, head_count, HD)
    )
    attn_full, lse_all = attend(queries, keys_rot, value_rows, prefix_seq)
    attn_low = attn_full.astype(jnp.bfloat16)
    attn_proj = lax.psum_scatter(
        product(attn_low, output_full).astype(jnp.bfloat16),
        "tensor",
        scatter_dimension=0,
        tiled=True,
    ).astype(jnp.float32)
    unit_two, factor_two = normalize(attn_proj)
    middle = residual + unit_two * gain_b
    unit_three, factor_three = normalize(middle)
    mlp_in = lax.all_gather(
        (unit_three * gain_c).astype(jnp.bfloat16), "tensor", axis=0, tiled=True
    )
    gate_act = product(mlp_in, gate_full)
    up_act = product(mlp_in, up_full)
    hidden = (jax.nn.silu(gate_act) * up_act).astype(jnp.bfloat16)
    mlp_proj = lax.psum_scatter(
        product(hidden, down_full).astype(jnp.bfloat16), "tensor", scatter_dimension=0, tiled=True
    ).astype(jnp.float32)
    unit_four, factor_four = normalize(mlp_proj)
    result = middle + unit_four * gain_d
    grad_out = cot_rows.astype(jnp.float32)
    post_mlp_part = jnp.sum(grad_out * unit_four, axis=0)
    grad_mlp = norm_back(grad_out * gain_d, unit_four, factor_four).astype(jnp.bfloat16)
    grad_mlp_all = lax.all_gather(grad_mlp, "tensor", axis=0, tiled=True)
    down_part = inner(hidden, grad_mlp_all)
    grad_hidden = outer_t(grad_mlp_all, down_full)
    sigma = jax.nn.sigmoid(gate_act)
    grad_gate = (grad_hidden * up_act * sigma * (1.0 + gate_act * (1.0 - sigma))).astype(
        jnp.bfloat16
    )
    grad_up = (grad_hidden * gate_act * sigma).astype(jnp.bfloat16)
    gate_part = inner(mlp_in, grad_gate)
    up_part = inner(mlp_in, grad_up)
    grad_mlp_in = lax.psum_scatter(
        (outer_t(grad_gate, gate_full) + outer_t(grad_up, up_full)).astype(jnp.bfloat16),
        "tensor",
        scatter_dimension=0,
        tiled=True,
    ).astype(jnp.float32)
    pre_mlp_part = jnp.sum(grad_mlp_in * unit_three, axis=0)
    grad_middle = grad_out + norm_back(grad_mlp_in * gain_c, unit_three, factor_three)
    post_attn_part = jnp.sum(grad_middle * unit_two, axis=0)
    grad_proj = norm_back(grad_middle * gain_b, unit_two, factor_two).astype(jnp.bfloat16)
    grad_proj_all = lax.all_gather(grad_proj, "tensor", axis=0, tiled=True)
    output_part = inner(attn_low, grad_proj_all)
    grad_attn = (
        outer_t(grad_proj_all, output_full).astype(jnp.bfloat16).reshape(row_total, head_count, HD)
    )
    grad_q, grad_k, grad_v = attend_back(
        queries, keys_rot, value_rows, lse_all, grad_attn, prefix_seq
    )
    grad_q_raw = (
        rotate_back(grad_q, cosine, sine_tab)
        .astype(jnp.bfloat16)
        .reshape(row_total, head_count * HD)
    )
    grad_k_raw = (
        rotate_back(grad_k, cosine, sine_tab)
        .astype(jnp.bfloat16)
        .reshape(row_total, head_count * HD)
    )
    grad_values = grad_v.astype(jnp.bfloat16).reshape(row_total, head_count * HD)
    query_part = inner(attn_in, grad_q_raw)
    key_part = inner(attn_in, grad_k_raw)
    value_part = inner(attn_in, grad_values)
    grad_attn_in_part = (
        outer_t(grad_q_raw, query_full)
        + outer_t(grad_k_raw, key_full)
        + outer_t(grad_values, value_full)
    )
    grad_attn_in = lax.psum_scatter(
        grad_attn_in_part.astype(jnp.bfloat16), "tensor", scatter_dimension=0, tiled=True
    ).astype(jnp.float32)
    pre_attn_part = jnp.sum(grad_attn_in * unit_one, axis=0)
    grad_residual = (grad_middle + norm_back(grad_attn_in * gain_a, unit_one, factor_one)).astype(
        jnp.bfloat16
    )
    adapter_part = inner(joined, grad_residual)
    grad_joined = outer_t(grad_residual, adapter_full)
    width = lat_rows.shape[1]
    latent_grad = grad_joined[:, :width].astype(jnp.bfloat16)
    embedding_grad = grad_joined[:, width:].astype(jnp.bfloat16)
    partials = (
        adapter_part,
        pre_attn_part,
        post_attn_part,
        pre_mlp_part,
        post_mlp_part,
        query_part,
        key_part,
        value_part,
        output_part,
        gate_part,
        up_part,
        down_part,
    )
    return (result.astype(jnp.bfloat16), latent_grad, embedding_grad, partials)


def local(
    latent,
    embedding,
    prefix_len,
    cotangent,
    adapter_w,
    pre_attn_gain,
    post_attn_gain,
    pre_mlp_gain,
    post_mlp_gain,
    query_w,
    key_w,
    value_w,
    output_w,
    gate_w,
    up_w,
    down_w,
):
    local_weights = (
        adapter_w,
        pre_attn_gain,
        post_attn_gain,
        pre_mlp_gain,
        post_mlp_gain,
        query_w,
        key_w,
        value_w,
        output_w,
        gate_w,
        up_w,
        down_w,
    )
    batches = latent.shape[0]
    layer_rows = []
    latent_rows = []
    embed_rows = []
    totals = None
    for micro in range(batches):
        current = gather_weights(local_weights)
        result, lat_grad, emb_grad, partials = micro_step(
            latent[micro], embedding[micro], prefix_len[micro], cotangent[micro], current
        )
        layer_rows.append(result)
        latent_rows.append(lat_grad)
        embed_rows.append(emb_grad)
        if totals is None:
            totals = partials
        else:
            totals = jax.tree.map(lambda left, right: left + right, totals, partials)
    adapter_grad, pre_attn_grad, post_attn_grad, pre_mlp_grad, post_mlp_grad = (
        lax.psum_scatter(totals[0], ("dp", "tensor"), scatter_dimension=0, tiled=True),
        lax.psum_scatter(totals[1], ("dp", "tensor"), scatter_dimension=0, tiled=True),
        lax.psum_scatter(totals[2], ("dp", "tensor"), scatter_dimension=0, tiled=True),
        lax.psum_scatter(totals[3], ("dp", "tensor"), scatter_dimension=0, tiled=True),
        lax.psum_scatter(totals[4], ("dp", "tensor"), scatter_dimension=0, tiled=True),
    )
    query_grad, key_grad, value_grad, output_grad = (
        lax.psum_scatter(
            totals[5].astype(jnp.bfloat16), "dp", scatter_dimension=0, tiled=True
        ).astype(jnp.float32),
        lax.psum_scatter(
            totals[6].astype(jnp.bfloat16), "dp", scatter_dimension=0, tiled=True
        ).astype(jnp.float32),
        lax.psum_scatter(
            totals[7].astype(jnp.bfloat16), "dp", scatter_dimension=0, tiled=True
        ).astype(jnp.float32),
        lax.psum_scatter(
            totals[8].astype(jnp.bfloat16), "dp", scatter_dimension=1, tiled=True
        ).astype(jnp.float32),
    )
    gate_grad, up_grad, down_grad = (
        lax.psum_scatter(
            totals[9].astype(jnp.bfloat16), "dp", scatter_dimension=0, tiled=True
        ).astype(jnp.float32),
        lax.psum_scatter(
            totals[10].astype(jnp.bfloat16), "dp", scatter_dimension=0, tiled=True
        ).astype(jnp.float32),
        lax.psum_scatter(
            totals[11].astype(jnp.bfloat16), "dp", scatter_dimension=1, tiled=True
        ).astype(jnp.float32),
    )
    return (
        jnp.stack(layer_rows),
        jnp.stack(latent_rows),
        jnp.stack(embed_rows),
        adapter_grad,
        pre_attn_grad,
        post_attn_grad,
        pre_mlp_grad,
        post_mlp_grad,
        query_grad,
        key_grad,
        value_grad,
        output_grad,
        gate_grad,
        up_grad,
        down_grad,
    )


ROWS_F, KEYS_F, ROWS_B, KEYS_B = 1024, 512, 512, 512
LOG2E = 1.4426950408889634
NEG = -1e30


def turn(values, cosine, signed_sine):
    return values * cosine + pltpu.roll(values, HD // 2, 1) * signed_sine


def visible(row_start, rows, key_start, keys, prefix_end):
    row_at = row_start + lax.broadcasted_iota(jnp.int32, (keys, rows), 1)
    key_at = key_start + lax.broadcasted_iota(jnp.int32, (keys, rows), 0)
    if prefix_end is None:
        return key_at <= row_at
    return (key_at <= row_at) | (key_at < prefix_end)


def attend_kernel(
    info, q_own, q_oth, k_own, k_oth, v_own, v_oth, cos_ref, sin_ref,
    attn_ref, lse_ref, q_ref, k_ref, v_ref, wide,
):
    side, prefix_end = info[0], info[1]
    half = q_own.shape[0]
    length = 2 * half
    factor = LOG2E * HD**-0.5
    for slot, (q_in, k_in, v_in) in enumerate(((q_own, k_own, v_own), (q_oth, k_oth, v_oth))):
        place = side if slot == 0 else 1 - side
        rows = pl.ds(pl.multiple_of(place * half, half), half)
        cosine, signed_sine = cos_ref[rows, :], sin_ref[rows, :]
        here = pl.ds(slot * half, half)
        q_ref[here, :] = turn(q_in[...], cosine, signed_sine).astype(jnp.bfloat16)
        k_ref[here, :] = turn(k_in[...], cosine, signed_sine).astype(jnp.bfloat16)
        v_ref[here, :] = v_in[...]
        wide[:HD, here] = jnp.transpose(v_in[...].astype(jnp.float32)).astype(jnp.bfloat16)
    wide[HD:, :] = jnp.ones((16, length), jnp.bfloat16)

    def stored(start, size):
        offset = lax.rem(start // half + side, 2) * half + start % half
        return pl.ds(pl.multiple_of(offset, size), size)

    for start in range(0, length, ROWS_F):
        mine = stored(start, ROWS_F)
        queries = q_ref[mine, :]
        top = None
        end = max(start + ROWS_F, half)
        for key_start in range(0, end, KEYS_F):
            keys = stored(key_start, KEYS_F)
            scores = outer_t(k_ref[keys, :], queries) * factor
            if key_start + KEYS_F - 1 > start:
                limit = prefix_end if key_start < half else None
                seen = visible(start, ROWS_F, key_start, KEYS_F, limit)
                scores = jnp.where(seen, scores, NEG)
            peak = jnp.max(scores, axis=0, keepdims=True)
            old, top = top, (peak if top is None else jnp.maximum(top, peak))
            weights = jnp.exp2(scores - top).astype(jnp.bfloat16)
            part = product(wide[:, keys], weights)
            total = part if old is None else total * jnp.exp2(old - top) + part
        denominator = total[HD : HD + 1, :]
        attn_ref[mine, :] = jnp.transpose(total[:HD, :] / denominator).astype(jnp.bfloat16)
        lse_ref[0, :, mine] = jnp.broadcast_to(top + jnp.log2(denominator), (8, ROWS_F))


def attend_back_kernel(
    info, q_ref, k_ref, v_ref, attn_ref, lse_ref, go_own, go_oth, cos_ref, sin_ref,
    grad_ref, go_ref, delta, dq,
):
    side, prefix_end = info[0], info[1]
    head = pl.program_id(0)
    heads = grad_ref.shape[1] // (3 * HD)
    half = go_own.shape[0]
    length = 2 * half
    factor = LOG2E * HD**-0.5
    scaling = HD**-0.5

    def stored(start, size):
        offset = lax.rem(start // half + side, 2) * half + start % half
        return pl.ds(pl.multiple_of(offset, size), size)

    def columns(kind):
        return pl.ds(pl.multiple_of((kind * heads + head) * HD, HD), HD)

    go_ref[:half, :] = go_own[...]
    go_ref[half:, :] = go_oth[...]
    for start in range(0, length, half):
        here = pl.ds(start, half)
        both = go_ref[here, :].astype(jnp.float32) * attn_ref[here, :].astype(jnp.float32)
        delta[:, here] = jnp.broadcast_to(
            jnp.sum(jnp.transpose(both), axis=0, keepdims=True), (8, half)
        )
    dq[...] = jnp.zeros_like(dq)

    for key_start in range(0, length, KEYS_B):
        keys = stored(key_start, KEYS_B)
        key_rows, values = k_ref[keys, :], v_ref[keys, :]
        grad_key = grad_value = None
        first = 0 if key_start < half else key_start // ROWS_B * ROWS_B
        for start in range(first, length, ROWS_B):
            rows = stored(start, ROWS_B)
            queries, grads = q_ref[rows, :], go_ref[rows, :]
            scores = outer_t(key_rows, queries) * factor - lse_ref[0, :1, rows]
            if key_start + KEYS_B - 1 > start:
                limit = prefix_end if key_start < half else None
                seen = visible(start, ROWS_B, key_start, KEYS_B, limit)
                scores = jnp.where(seen, scores, NEG)
            weights = jnp.exp2(scores)
            slope = outer_t(values, grads) - delta[:1, rows]
            narrow = (weights * slope).astype(jnp.bfloat16)
            value_part = product(weights.astype(jnp.bfloat16), grads)
            key_part = product(narrow, queries)
            grad_value = value_part if grad_value is None else grad_value + value_part
            grad_key = key_part if grad_key is None else grad_key + key_part
            dq[rows, :] += inner(narrow, key_rows)
        place = pl.ds(key_start, KEYS_B)
        back = turn(grad_key * scaling, cos_ref[place, :], -sin_ref[place, :])
        grad_ref[keys, columns(1)] = back.astype(jnp.bfloat16)
        grad_ref[keys, columns(2)] = grad_value.astype(jnp.bfloat16)

    for start in range(0, length, half):
        rows, place = stored(start, half), pl.ds(start, half)
        back = turn(dq[rows, :] * scaling, cos_ref[place, :], -sin_ref[place, :])
        grad_ref[rows, columns(0)] = back.astype(jnp.bfloat16)


def head_columns(rows, shift=0):
    return pl.BlockSpec((rows, HD), lambda head, info: (0, head + shift))


def fixed(rows, columns):
    return pl.BlockSpec((rows, columns), lambda head, info: (0, 0))


def attend_half(info, qk_own, qk_oth, v_own, v_oth, tables):
    half = qk_own.shape[0]
    heads = v_own.shape[1] // HD
    length = 2 * half
    low = jax.ShapeDtypeStruct((length, heads * HD), jnp.bfloat16)
    pairs = heads * length * length * 0.6
    return pl.pallas_call(
        attend_kernel,
        grid_spec=pltpu.PrefetchScalarGridSpec(
            num_scalar_prefetch=1,
            grid=(heads,),
            in_specs=[
                head_columns(half), head_columns(half),
                head_columns(half, heads), head_columns(half, heads),
                head_columns(half), head_columns(half),
                fixed(length, HD), fixed(length, HD),
            ],
            out_specs=[
                head_columns(length),
                pl.BlockSpec((1, 8, length), lambda head, info: (head, 0, 0)),
                head_columns(length), head_columns(length), head_columns(length),
            ],
            scratch_shapes=[
                pltpu.VMEM((HD + 16, length), jnp.bfloat16),
            ],
        ),
        out_shape=(low, jax.ShapeDtypeStruct((heads, 8, length), jnp.float32), low, low, low),
        cost_estimate=pl.CostEstimate(
            flops=int(pairs * 8 * HD), bytes_accessed=int(40 * length * heads * HD), transcendentals=int(pairs)
        ),
        name="attend",
    )(info, qk_own, qk_oth, qk_own, qk_oth, v_own, v_oth, *tables)


def attend_back_half(info, saved, go_own, go_oth, tables):
    attn, lse, queries, keys_rot, value_rows = saved
    half = go_own.shape[0]
    heads = go_own.shape[1] // HD
    length = 2 * half
    pairs = heads * length * length * 0.6
    return pl.pallas_call(
        attend_back_kernel,
        grid_spec=pltpu.PrefetchScalarGridSpec(
            num_scalar_prefetch=1,
            grid=(heads,),
            in_specs=[
                head_columns(length), head_columns(length), head_columns(length), head_columns(length),
                pl.BlockSpec((1, 8, length), lambda head, info: (head, 0, 0)),
                head_columns(half), head_columns(half),
                fixed(length, HD), fixed(length, HD),
            ],
            out_specs=fixed(length, 3 * heads * HD),
            scratch_shapes=[
                pltpu.VMEM((length, HD), jnp.bfloat16),
                pltpu.VMEM((8, length), jnp.float32),
                pltpu.VMEM((length, HD), jnp.float32),
            ],
        ),
        out_shape=jax.ShapeDtypeStruct((length, 3 * heads * HD), jnp.bfloat16),
        cost_estimate=pl.CostEstimate(
            flops=int(pairs * 20 * HD), bytes_accessed=int(16 * length * heads * HD), transcendentals=int(pairs)
        ),
        name="attend_back",
    )(info, queries, keys_rot, value_rows, attn, lse, go_own, go_oth, *tables)


def plain(values):
    return with_layout_constraint(values, Layout(major_to_minor=tuple(range(values.ndim))))


def swap(values):
    return lax.ppermute(values, "tensor", [(0, 1), (1, 0)])


def low(values):
    return values.astype(jnp.bfloat16)


def packed(pieces):
    whole = jnp.zeros((pieces[0].shape[0], sum(piece.shape[1] for piece in pieces)), pieces[0].dtype)
    start = 0
    for piece in pieces:
        whole = lax.dynamic_update_slice(whole, piece, (0, start))
        start += piece.shape[1]
    return whole


def scattered(parts):
    return lax.psum_scatter(parts, "dp", scatter_dimension=0, tiled=True)


def halves_summed(mine, side):
    width = mine.shape[1] // 2
    lower, upper = mine[:, :width], mine[:, width:]
    sent = jnp.where(side == 0, upper, lower)
    kept = jnp.where(side == 0, lower, upper)
    return kept.astype(jnp.float32) + swap(sent).astype(jnp.float32)


def after(values, *others):
    return lax.optimization_barrier((values, *others))[0]


def fast_local(
    latent, embedding, prefix_len, cotangent, adapter_w, pre_attn_gain, post_attn_gain,
    pre_mlp_gain, post_mlp_gain, query_w, key_w, value_w, output_w, gate_w, up_w, down_w,
):
    side = lax.axis_index("tensor")
    dp_size, both = lax.axis_size("dp"), ("dp", "tensor")
    half, width = latent.shape[1:]
    shard = adapter_w.shape[0]
    gain_len = pre_attn_gain.shape[0]
    quarter = query_w.shape[1]
    inner_len = gate_w.shape[1]

    gains_row = jnp.concatenate([pre_attn_gain, post_attn_gain, pre_mlp_gain, post_mlp_gain])
    gains_block = jnp.pad(gains_row[None, :], ((0, shard - 1), (0, 0)))
    first = lax.all_gather(jnp.concatenate([adapter_w, gains_block], axis=1), both, axis=0, tiled=True)
    attn_w = lax.all_gather(
        jnp.concatenate([query_w, key_w, value_w], axis=1), ("tensor", "dp"), axis=0, tiled=True
    ).reshape(2, width, -1)
    mlp_w = lax.all_gather(
        jnp.concatenate([gate_w, up_w, down_w.T, output_w.T], axis=1), ("tensor", "dp"), axis=0, tiled=True
    ).reshape(2, width, -1)
    adapter_top, adapter_bottom = first[:width, :width], first[width:, :width]
    gains = first[::shard, width:].reshape(-1, 4, gain_len).transpose(1, 0, 2).reshape(4, width)
    gain_a, gain_b, gain_c, gain_d = (gains[i].astype(jnp.float32) for i in range(4))

    info = jnp.stack([side.astype(jnp.int32), jnp.where(side == 0, prefix_len[0, 0], prefix_len[1, 0])])
    half_dim = HD // 2
    inv_freq = THETA ** (-(jnp.arange(half_dim, dtype=jnp.float32) * 2.0 / HD))
    angles = jnp.arange(2 * half, dtype=jnp.float32)[:, None] * inv_freq[None, :]
    cosine, sine = jnp.cos(angles), jnp.sin(angles)
    tables = (jnp.concatenate([cosine, cosine], axis=1), jnp.concatenate([-sine, sine], axis=1))

    def pick(values, index):
        return plain(lax.dynamic_index_in_dim(values, index, 0, keepdims=False))

    order = (side, 1 - side)
    lat = [pick(latent, i) for i in order]
    emb = [pick(embedding, i) for i in order]
    cot = [pick(cotangent, i) for i in order]

    def enter(slot):
        residual = plain(product(lat[slot], adapter_top) + product(emb[slot], adapter_bottom))
        unit, factor = normalize(residual)
        return residual, unit, factor, low(unit * gain_a)

    res_o, unit_one_o, factor_one_o, attn_in_sent = enter(1)
    attn_in_oth = swap(attn_in_sent)
    res_m, unit_one_m, factor_one_m, attn_in_own = enter(0)

    def project(rows, part):
        weights = attn_w[part]
        return (
            product(rows, weights[:, : 2 * quarter]),
            low(product(rows, weights[:, 2 * quarter : 3 * quarter])),
        )

    own = [project(attn_in_own, part) for part in range(2)]
    oth = [project(attn_in_oth, part) for part in range(2)]
    saved = [
        attend_half(info, own[p][0], oth[p][0], own[p][1], oth[p][1], tables) for p in range(2)
    ]
    out_w = [mlp_w[p][:, 3 * inner_len :] for p in range(2)]

    def project_out(rows):
        return outer_t(saved[0][0][rows], out_w[0]) + outer_t(saved[1][0][rows], out_w[1])

    proj_o = swap(low(project_out(slice(half, None))))
    proj_m = low(project_out(slice(0, half))).astype(jnp.float32)

    gate_w_all = [mlp_w[p][:, :inner_len] for p in range(2)]
    up_w_all = [mlp_w[p][:, inner_len : 2 * inner_len] for p in range(2)]
    down_w_all = [mlp_w[p][:, 2 * inner_len : 3 * inner_len] for p in range(2)]

    def feed(residual, attn_proj, cot_rows):
        unit_two, factor_two = normalize(attn_proj)
        middle = residual + unit_two * gain_b
        unit_three, factor_three = normalize(middle)
        mlp_in = low(unit_three * gain_c)
        acts = []
        mlp_proj = None
        for p in range(2):
            gate_act = product(mlp_in, gate_w_all[p])
            up_act = product(mlp_in, up_w_all[p])
            hidden = low(jax.nn.silu(gate_act) * up_act)
            acts.append((gate_act, up_act, hidden))
            part = outer_t(hidden, down_w_all[p])
            mlp_proj = part if mlp_proj is None else mlp_proj + part
        unit_four, factor_four = normalize(mlp_proj)
        result = plain(low(middle + unit_four * gain_d))
        grad_out = cot_rows.astype(jnp.float32)
        post_mlp_part = jnp.sum(grad_out * unit_four, axis=0)
        grad_mlp = low(norm_back(grad_out * gain_d, unit_four, factor_four))
        grads = []
        grad_mlp_in = None
        for p in range(2):
            gate_act, up_act, hidden = acts[p]
            grad_hidden = product(grad_mlp, down_w_all[p])
            sigma = jax.nn.sigmoid(gate_act)
            grad_gate = low(grad_hidden * up_act * sigma * (1.0 + gate_act * (1.0 - sigma)))
            grad_up = low(grad_hidden * gate_act * sigma)
            grads.append((grad_gate, grad_up, hidden))
            part = outer_t(grad_gate, gate_w_all[p]) + outer_t(grad_up, up_w_all[p])
            grad_mlp_in = part if grad_mlp_in is None else grad_mlp_in + part
        pre_mlp_part = jnp.sum(grad_mlp_in * unit_three, axis=0)
        grad_middle = grad_out + norm_back(grad_mlp_in * gain_c, unit_three, factor_three)
        post_attn_part = jnp.sum(grad_middle * unit_two, axis=0)
        grad_proj = low(norm_back(grad_middle * gain_b, unit_two, factor_two))
        return result, grad_middle, grad_proj, mlp_in, grad_mlp, grads, (
            post_attn_part, pre_mlp_part, post_mlp_part,
        )

    result_m, grad_middle_m, grad_proj_own, mlp_in_m, grad_mlp_m, grads_m, sums_m = feed(
        res_m, proj_m, cot[0]
    )
    proj_o, grad_mlp_m = lax.optimization_barrier((proj_o, grad_mlp_m))
    result_o, grad_middle_o, grad_proj_sent, mlp_in_o, grad_mlp_o, grads_o, sums_o = feed(
        res_o, proj_o.astype(jnp.float32), cot[1]
    )
    grad_proj_oth = swap(grad_proj_sent)
    down_pack = packed(
        [low(inner(grad_mlp_m, grads_m[p][2]) + inner(grad_mlp_o, grads_o[p][2])) for p in range(2)]
    )
    mlp_cols = []
    for p in range(2):
        for i in range(2):
            mlp_cols.append(low(inner(mlp_in_m, grads_m[p][i]) + inner(mlp_in_o, grads_o[p][i])))
    mlp_pack = packed(mlp_cols)
    down_mine = scattered(down_pack)
    grad_proj_own, grad_proj_oth, mlp_pack, down_pack = lax.optimization_barrier(
        (grad_proj_own, grad_proj_oth, mlp_pack, down_pack)
    )
    mlp_mine = scattered(after(mlp_pack, down_mine))

    grad_qkv = []
    for p in range(2):
        go_own = low(product(grad_proj_own, out_w[p]))
        go_oth = low(product(grad_proj_oth, out_w[p]))
        grad_qkv.append(attend_back_half(info, saved[p], go_own, go_oth, tables))

    in_w = attn_w

    def grad_in(rows):
        return outer_t(grad_qkv[0][rows], in_w[0]) + outer_t(grad_qkv[1][rows], in_w[1])

    grad_in_o = swap(low(grad_in(slice(half, None))))
    grad_in_m = low(grad_in(slice(0, half))).astype(jnp.float32)
    attn_cols = []
    for p in range(2):
        mine, others = slice(0, half), slice(half, None)
        attn_cols.append(
            low(inner(attn_in_own, grad_qkv[p][mine]) + inner(attn_in_oth, grad_qkv[p][others]))
        )
        attn_cols.append(
            low(inner(grad_proj_own, saved[p][0][mine]) + inner(grad_proj_oth, saved[p][0][others]))
        )
    attn_pack = packed(attn_cols)

    def leave(grad_attn_in, unit_one, factor_one, grad_middle):
        part = jnp.sum(grad_attn_in * unit_one, axis=0)
        grad_residual = low(grad_middle + norm_back(grad_attn_in * gain_a, unit_one, factor_one))
        return (
            grad_residual, part,
            plain(low(outer_t(grad_residual, adapter_top))), plain(low(outer_t(grad_residual, adapter_bottom))),
        )

    grad_res_m, pre_m, lat_grad_m, emb_grad_m = leave(grad_in_m, unit_one_m, factor_one_m, grad_middle_m)
    grad_in_o, attn_pack, grad_res_m = lax.optimization_barrier((grad_in_o, attn_pack, grad_res_m))
    attn_mine = scattered(after(attn_pack, mlp_mine))
    grad_in_o = grad_in_o.astype(jnp.float32)
    grad_res_o, pre_o, lat_grad_o, emb_grad_o = leave(grad_in_o, unit_one_o, factor_one_o, grad_middle_o)
    top = low(inner(lat[0], grad_res_m) + inner(lat[1], grad_res_o))
    bottom = low(inner(emb[0], grad_res_m) + inner(emb[1], grad_res_o))
    gain_sums = jnp.stack([pre_m + pre_o] + [sums_m[i] + sums_o[i] for i in range(3)])
    gain_sums = low(gain_sums).reshape(4, -1, gain_len).transpose(1, 0, 2).reshape(-1, 1, 4 * gain_len)
    gain_sums = jnp.pad(gain_sums, ((0, 0), (0, shard - 1), (0, 0))).reshape(-1, 4 * gain_len)
    last = jnp.concatenate([jnp.concatenate([top, bottom], axis=0), gain_sums], axis=1)
    down_total = halves_summed(down_mine, side)
    mlp_total = halves_summed(mlp_mine, side)
    attn_total = halves_summed(attn_mine, side)
    last = scattered(after(last, attn_mine))
    sent = jnp.where(side == 0, last[shard:], last[:shard])
    kept = jnp.where(side == 0, last[:shard], last[shard:])
    last = kept.astype(jnp.float32) + swap(sent).astype(jnp.float32)
    gain_grads = [last[0, width + i * gain_len : width + (i + 1) * gain_len] for i in range(4)]

    def join(mine, others):
        return jnp.stack([jnp.where(side == 0, mine, others), jnp.where(side == 0, others, mine)])

    return (
        join(result_m, result_o),
        join(lat_grad_m, lat_grad_o),
        join(emb_grad_m, emb_grad_o),
        last[:, :width],
        *gain_grads,
        attn_total[:, :quarter],
        attn_total[:, quarter : 2 * quarter],
        attn_total[:, 2 * quarter : 3 * quarter],
        attn_total[:, 3 * quarter :].T,
        mlp_total[:, :inner_len],
        mlp_total[:, inner_len:],
        down_total.T,
    )


def choose(*arguments):
    latent, prefix_len, query_w = arguments[0], arguments[2], arguments[9]
    paired = lax.axis_size("tensor") == 2 and latent.shape[0] == 2
    whole = 2 * latent.shape[1] == LEN and prefix_len.shape[1] == 1 and query_w.shape[1] % HD == 0
    return fast_local(*arguments) if paired and whole else local(*arguments)


def solution(mesh):
    placed = (
        P(None, ("dp", "tensor"), None),
        P(None, ("dp", "tensor"), None),
        P(None, "dp"),
        P(None, ("dp", "tensor"), None),
        P(("dp", "tensor"), None),
        P(("dp", "tensor")),
        P(("dp", "tensor")),
        P(("dp", "tensor")),
        P(("dp", "tensor")),
        P("dp", "tensor"),
        P("dp", "tensor"),
        P("dp", "tensor"),
        P("tensor", "dp"),
        P("dp", "tensor"),
        P("dp", "tensor"),
        P("tensor", "dp"),
    )
    return jax.shard_map(
        choose,
        mesh=mesh,
        in_specs=placed,
        out_specs=(
            P(None, ("dp", "tensor"), None),
            P(None, ("dp", "tensor"), None),
            P(None, ("dp", "tensor"), None),
            P(("dp", "tensor"), None),
            P(("dp", "tensor")),
            P(("dp", "tensor")),
            P(("dp", "tensor")),
            P(("dp", "tensor")),
            P("dp", "tensor"),
            P("dp", "tensor"),
            P("dp", "tensor"),
            P("tensor", "dp"),
            P("dp", "tensor"),
            P("dp", "tensor"),
            P("tensor", "dp"),
        ),
        check_vma=False,
    )
```
